32 devices in a mesh: row: 8 (over z, x), col: 4 (over y, core).
Axes of the slice: x: 2, y: 2, z: 4, core: 2. Of those that a mesh axis runs over, the one named last changes fastest.
Arguments:
- gradients: bfloat16 [32, 1024, 5120], P(('row', 'col')), may hold values from -24 to 24
- bucket_lengths: int32 [16], replicated, may hold values from 1 to 128, 1024 in all
- owner_offset: int32 [8], replicated, may hold values from 0 to 3
- clip_rms: float32 [1], replicated, may hold values from 0.15 to 0.4
Outputs:
- clipped_shard: float32 [1024, 5120], P('row', 'col')
- bucket_rms: float32 [16], replicated
The draws below stay inside these ranges and needn't reach their ends.
Inputs may be any that keep to these rules, and one draw needn't show every extreme that they name: `bucket_lengths`: the buckets cover all 1024 rows; the largest has exactly 128 rows.
All inputs are finite; a program needn't handle non-finite values.
Results may differ from the reference program's by a relative error of at most 0.0003.
Values sent between devices are 32-bit elements; how exact they have to be, the bound alone decides.
A program may use at most 128 MiB of HBM per device.

```python
import math
import jax
import jax.numpy as jnp
import numpy as np
from jax import lax

D = 5120
ROWS = 1024
NBUCK = 16
MOSTB = 128
N_ROW = 8
N_COL = 4


def draw_gradients(key, part):
    devices = N_ROW * N_COL
    noise_key = jax.random.fold_in(key, 11)
    scale_key = jax.random.fold_in(key, 12)
    row_scale = jnp.exp(jax.random.uniform(scale_key, (ROWS,), jnp.float32, jnp.log(0.25), jnp.log(4.0)))
    noise = jax.random.normal(noise_key, (devices, ROWS, D), jnp.float32)
    values = 4.0 * row_scale[None, :, None] * noise
    return jnp.clip(values, -24.0, 24.0).astype(jnp.bfloat16)


def set_ends(result, stream_key, smallest, largest):
    extent = result.shape
    spot = [jax.random.randint(jax.random.fold_in(stream_key, axis), (), 0, extent[axis]) for axis in range(len(extent))]
    result = result.at[tuple(spot)].set(smallest)
    longest = extent.index(max(extent))
    spot[longest] = (spot[longest] + 1) % extent[longest]
    return result.at[tuple(spot)].set(largest)


def profile(count, total, limit, lean):
    portions = [(1 << 20) // math.isqrt(grade ** lean) + 1 for grade in range(2, count + 1)]
    rest, counts = total - limit - (count - 1), [1] * (count - 1)
    while rest > 0:
        movable = [i for i in range(count - 1) if counts[i] < limit]
        pool, budget = sum([portions[i] for i in movable]), rest
        for i in movable:
            extra = min(limit - counts[i], max(1, budget * portions[i] // pool), rest)
            counts[i] = counts[i] + extra
            rest = rest - extra
    return np.array([limit] + counts)


def uneven_parts(stream_key, amount, total, reach, lean):
    if amount == 2:
        one = jax.random.randint(stream_key, (), max(1, total - reach), min(reach, total - 1) + 1)
        return jnp.stack([one, total - one])
    lengths = jnp.asarray(profile(amount, total, reach, lean), jnp.int32)
    couples = (amount - 1) // 2
    source_of, receiver = lengths[1:1 + 2 * couples:2], lengths[2:2 + 2 * couples:2]
    slack = jnp.minimum(source_of - 1, reach - receiver)
    shifted = jax.random.randint(jax.random.fold_in(stream_key, 1), (couples,), 0, 1 << 20) % (slack + 1)
    lengths = lengths.at[1:1 + 2 * couples:2].set(source_of - shifted).at[2:2 + 2 * couples:2].set(receiver + shifted)
    return lengths[jax.random.permutation(jax.random.fold_in(stream_key, 2), amount)]


def setup_inputs(seed: int = 0) -> dict:
    keys = jax.random.split(jax.random.key(seed), 5)
    return {
        "gradients": draw_gradients(jax.random.fold_in(keys[4], 71), 0),
        "bucket_lengths": uneven_parts(keys[1], NBUCK, ROWS, MOSTB, 2).astype(jnp.int32),
        "owner_offset": set_ends(jax.random.randint(keys[2], (N_ROW,), 0, N_COL), jax.random.fold_in(keys[2], 1), 0, N_COL - 1).astype(jnp.int32),
        "clip_rms": jnp.clip(jax.random.uniform(keys[3], (1,), jnp.float32, 0.15, 0.4), 0.15, 0.4),
    }


def reference(gradients, bucket_lengths, owner_offset, clip_rms):
    devices = N_ROW * N_COL

    def accumulate(index, total):
        return total + gradients[index].astype(jnp.float32)
    summed = lax.fori_loop(0, devices, accumulate, jnp.zeros((ROWS, D), jnp.float32))
    averaged = summed / devices
    ends = jnp.cumsum(bucket_lengths).astype(jnp.int32)
    starts = (ends - bucket_lengths).astype(jnp.int32)
    row_ids = jnp.arange(ROWS, dtype=jnp.int32)
    member = ((row_ids[:, None] >= starts[None, :]) & (row_ids[:, None] < ends[None, :])).astype(jnp.float32)
    row_squares = lax.optimization_barrier(jnp.sum(averaged * averaged, axis=1))
    bucket_squares = lax.optimization_barrier(jnp.sum(row_squares[:, None] * member, axis=0))
    overall = jnp.sqrt(jnp.sum(bucket_squares) / (ROWS * D))
    factor = clip_rms[0] / jnp.maximum(overall, clip_rms[0])
    clipped = (averaged * factor).reshape(N_ROW, ROWS // N_ROW, D)
    shifts = (owner_offset * (D // N_COL)).astype(jnp.int32)

    def turn(block, shift):
        return jnp.roll(block, -shift, axis=1)
    clipped_shard = jax.vmap(turn)(clipped, shifts).reshape(ROWS, D)
    bucket_rms = jnp.sqrt(bucket_squares / (bucket_lengths.astype(jnp.float32) * D))
    return (clipped_shard, bucket_rms)
```

```python
import functools

import jax
import jax.numpy as jnp
from jax import lax
from jax.experimental import pallas as pl
from jax.experimental.pallas import tpu as pltpu
from jax.sharding import PartitionSpec as P

MESH = pl.DeviceIdType.MESH
F32 = jnp.float32
ROWS = 16
COLS = 256
LANES = 3
INNER = 16
PARTS = 2
PLACES = (
    (1.08, 1.67, 1.70),
    (3.85, 3.82, 3.33),
    (6.25, 5.64, 6.04),
    (7.90, 7.35, 7.55),
    (10.61, 9.66, 10.24),
)


def plan(bits):
    places = list(PLACES[:4])
    while len(places) < bits:
        places.append(tuple(p + 1.5 for p in places[-1]))
    places.append(tuple(max(a, b + 1.5) for a, b in zip(PLACES[4], places[-1])))
    events = [(p % 1, s + 1, l, int(p // 1)) for s, row in enumerate(places) for l, p in enumerate(row)]
    spans = [[b - a for a, b in zip(x, y)] for x, y in zip([(0.0,) * LANES] + places, places)]
    rings = [max(2 * (int(d // 1) + 1) for d in row) for row in spans]
    return sorted(events), max(e[3] for e in events), rings


def kernel(n_row, n_col, bits, g_ref, len_hbm, off_hbm, clip_hbm, out_ref, stat_ref, src, head, *rest):
    sent, rest = rest[:LANES], rest[LANES:]
    sums, rest = [rest[l * (bits + 1) : (l + 1) * (bits + 1)] for l in range(LANES)], rest[LANES * (bits + 1) :]
    acc, bounds, mine, slots, len_ref, off_ref, clip_ref, load_sem, small_sem, *rest = rest
    sends, recvs, (both,) = rest[:LANES], rest[LANES : 2 * LANES], rest[2 * LANES :]
    events, deepest, rings = plan(bits)
    chunks = [s.shape[0] for s in sent]
    blocks = 1 << bits
    devices = n_row * n_col
    _, _, rows, w = src.shape
    width = w * n_col
    across = w // COLS
    row, col = lax.axis_index("row"), lax.axis_index("col")
    core = col % 2
    me = row * n_col + col
    small = [
        pltpu.make_async_copy(a, b, small_sem.at[i])
        for i, (a, b) in enumerate(((off_hbm, off_ref), (len_hbm, len_ref), (clip_hbm, clip_ref)))
    ]
    early = [
        pltpu.make_async_copy(g_ref.at[:, pl.ds(0, ROWS), pl.ds(j * w, LANES * COLS)], head.at[j], load_sem.at[j])
        for j in range(n_col)
    ]
    late = [
        pltpu.make_async_copy(g_ref.at[:, :, pl.ds(j * w, w)], src.at[j], load_sem.at[n_col + j])
        for j in range(n_col)
    ]
    for c in small[:1] + early + small[1:] + late:
        c.start()

    def turn(value, bit):
        return 1 - 2 * ((value >> bit) % 2)

    def flip(value, bit):
        return value + turn(value, bit) * (1 << bit)

    def peer(dim):
        return (row, flip(col, 1)) if dim == "y" else (flip(row, dim), col)

    high = list(range(2, bits - 1))
    orders = ([1, "xy", "yx"] + high, [0, "y", 1] + high, ["y", 0, 1] + high)

    def target(s, l, k):
        if s == 0:
            return (row, flip(col, 0))
        dim = orders[l][s - 1]
        if dim in ("xy", "yx"):
            pick = k % 2 if dim == "yx" else 1 - k % 2
            return (row + pick * turn(row, 0), col + (1 - pick) * turn(col, 1) * 2)
        return peer(dim)

    barrier = pltpu.get_barrier_semaphore()
    peers = [(row, flip(col, 0))] + [peer(d) for d in [0, "y", 1] + high]
    for other in peers:
        pl.semaphore_signal(barrier, inc=1, device_id=other, device_id_type=MESH)

    small[0].wait()

    def remote(a, b, s, r, dev):
        return pltpu.make_async_remote_copy(
            src_ref=a, dst_ref=b, send_sem=s, recv_sem=r, device_id=dev, device_id_type=MESH
        )

    def copy(s, l, k):
        half = blocks >> s
        a = sent[l].at[k] if s == 0 else sums[l][s - 1].at[k, pl.ds(half, half)]
        at = sum(rings[:s]) + k % rings[s]
        return remote(a, sums[l][s].at[k], sends[l].at[s], recvs[l].at[at], target(s, l, k))

    def unit(l, k):
        u = k * LANES + l
        return u, pl.multiple_of((u // across) * ROWS, ROWS), pl.multiple_of((u % across) * COLS, COLS)

    def spot(i, l, k):
        flips = {}
        for j, dim in enumerate(orders[l]):
            flips[dim] = (i >> (bits - 1 - j)) % 2
        if "xy" in flips:
            odd = k % 2
            flips[0] = flips["xy"] * (1 - odd) + flips["yx"] * odd
            flips["y"] = flips["yx"] * (1 - odd) + flips["xy"] * odd
        r = 0
        for b in range(bits - 1):
            r = r + (((row >> b) + flips[b]) % 2) * (1 << b)
        return r, (col // 2 + flips["y"]) % 2

    def each(lo, hi, fn):
        if hi - lo <= INNER:
            for i in range(lo, hi):
                fn(i)
        else:

            @pl.loop(0, (hi - lo) // INNER)
            def _(outer):
                for i in range(INNER):
                    fn(lo + outer * INNER + i)

    def piece(start, top, base, r, c, q):
        origin = lax.rem(c + off_ref[r], n_col)
        if start:
            return head[origin, r, :, pl.ds(base + q * 128, 128)].astype(F32)
        begin = pl.multiple_of(base + q * 128, 128)
        return src[origin, r, pl.ds(top, ROWS), pl.ds(begin, 128)].astype(F32)

    def convert(l, k, start=False):
        _, top, base = unit(l, k)
        base = l * COLS if start else base

        def fill(i):
            r, yd = spot(i, l, k)
            for q in range(COLS // 128):
                sent[l][k, i, :, q * 128 : (q + 1) * 128] = piece(start, top, base, r, yd * 2 + 1 - core, q)

        each(0, blocks, fill)

    def first(l, k, start=False):
        copy(0, l, k).wait_recv()
        _, top, base = unit(l, k)
        base = l * COLS if start else base

        def fold(i):
            r, yd = spot(i, l, k)
            for q in range(COLS // 128):
                sums[l][0][k, i, :, q * 128 : (q + 1) * 128] += piece(start, top, base, r, yd * 2 + core, q)

        each(blocks // 2, blocks, fold)
        copy(1, l, k).start()
        each(0, blocks // 2, fold)

    def middle(s, l, k):
        copy(s - 1, l, k).wait_recv()
        half = blocks >> s

        @pl.loop(half, 2 * half, unroll=min(2, half))
        def _(i):
            sums[l][s - 1][k, i] += sums[l][s - 2][k, i]

        copy(s, l, k).start()

        @pl.loop(0, half, unroll=min(2, half))
        def _(i):
            sums[l][s - 1][k, i] += sums[l][s - 2][k, i]

    def finish(l, k):
        copy(bits, l, k).wait_recv()
        _, top, base = unit(l, k)
        v = (sums[l][bits][k, 0] + sums[l][bits - 1][k, 0]) * (1.0 / devices)
        out_ref[pl.ds(top, ROWS), pl.ds(base, COLS)] = v
        v = v * v
        total = v[:, 0:128]
        for q in range(128, COLS, 128):
            total = total + v[:, q : q + 128]
        ids = lax.broadcasted_iota(jnp.int32, (ROWS, 128), 0) + row * rows + top
        after = jnp.clip(ids - bounds[0] + 1, 0, 1)
        before = jnp.clip(bounds[1] - ids, 0, 1)
        acc[...] += (after * before).astype(F32) * jnp.sum(total, axis=1, keepdims=True)

    def step(s, l, k):
        if s == 1:
            first(l, k)
        elif s <= bits:
            middle(s, l, k)
        else:
            finish(l, k)

    for c in early:
        c.wait()
    for l in range(LANES):
        convert(l, 0, True)

    small[1].wait()
    small[2].wait()
    lane = lax.broadcasted_iota(jnp.int32, (1, 128), 1)
    starts = jnp.zeros((1, 128), jnp.int32)
    lengths = jnp.zeros((1, 128), jnp.int32)
    begin = jnp.int32(0)
    for b in range(len_ref.shape[0]):
        starts = jnp.where(lane == b, begin, starts)
        lengths = jnp.where(lane == b, len_ref[b], lengths)
        begin = begin + len_ref[b]
    bounds[0] = starts
    bounds[1] = starts + lengths
    bounds[2] = lengths
    acc[...] = jnp.zeros_like(acc)

    pl.semaphore_wait(barrier, len(peers))
    for l in range(LANES):
        copy(0, l, 0).start()
    for l in range(LANES):
        first(l, 0, True)
    for c in late:
        c.wait()

    @pl.loop(1, chunks[0] + deepest)
    def _(t):
        for l in range(LANES):

            @pl.when(t < chunks[l])
            def _():
                convert(l, t)
                copy(0, l, t).start()

        for _, s, l, lag in events:

            @pl.when((t >= lag + (1 if s == 1 else 0)) & (t < chunks[l] + lag))
            def _():
                step(s, l, t - lag)

    local = jnp.sum(acc[...], axis=0, keepdims=True)
    mine[...] = local
    slots[me] = local

    def share(mask):
        other = me
        for b in range(bits + 1):
            if (mask >> b) % 2:
                other = flip(other, b)
        return remote(mine, slots.at[me], both.at[0], both.at[1], (other // n_col, other % n_col))

    for mask in range(devices - 1, 0, -1):
        share(mask).start()

    for l in range(LANES):
        for s in range(bits + 1):
            half = blocks >> s
            a = sent[l] if s == 0 else sums[l][s - 1].at[:, pl.ds(half, half)]
            pltpu.make_async_copy(a, a, sends[l].at[s]).wait()

    others = slots.at[pl.ds(0, devices - 1)]
    pltpu.make_async_copy(others, others, both.at[1]).wait()

    squares = slots[0]
    for i in range(1, devices):
        squares = squares + slots[i]
    overall = jnp.sqrt(jnp.sum(squares, axis=1, keepdims=True) / (n_row * rows * width))
    clip = clip_ref[0]
    factor = clip / jnp.maximum(overall, clip)
    rms = jnp.sqrt(squares / (jnp.maximum(bounds[2], 1).astype(F32) * width))
    stat_ref[0] = jnp.broadcast_to(factor, (8, 128))
    stat_ref[1] = jnp.broadcast_to(rms, (8, 128))
    pltpu.make_async_copy(others, others, both.at[0]).wait()


def scale(avg_ref, stat_ref, out_hbm, rms_hbm, out, rms, sem):
    rms[...] = stat_ref[1, 0:1, : rms.shape[1]]
    last = pltpu.make_async_copy(rms, rms_hbm, sem.at[0])
    last.start()
    factor = stat_ref[0, 0:1, 0:1]
    part = avg_ref.shape[0] // PARTS
    copies = []
    for i in range(PARTS):
        at = pl.ds(i * part, part)
        out[at] = avg_ref[at] * factor
        copies.append(pltpu.make_async_copy(out.at[at], out_hbm.at[at], sem.at[i + 1]))
        copies[-1].start()
    for c in copies:
        c.wait()
    last.wait()


def shards(n_row, n_col, gradients, bucket_lengths, owner_offset, clip_rms):
    _, total_rows, width = gradients.shape
    rows, w = total_rows // n_row, width // n_col
    devices = n_row * n_col
    bits = devices.bit_length() - 2
    blocks = 1 << bits
    units = rows // ROWS * (w // COLS)
    chunks = [(units - l + LANES - 1) // LANES for l in range(LANES)]
    vmem, smem = pltpu.VMEM, pltpu.SMEM
    dma = pltpu.SemaphoreType.DMA
    averaged, stats = pl.pallas_call(
        functools.partial(kernel, n_row, n_col, bits),
        out_shape=(
            jax.ShapeDtypeStruct((rows, w), F32),
            jax.ShapeDtypeStruct((2, 8, 128), F32),
        ),
        in_specs=[pl.BlockSpec(memory_space=pltpu.HBM)] * 4,
        out_specs=[pl.BlockSpec(memory_space=vmem)] * 2,
        scratch_shapes=[
            vmem((n_col, n_row, rows, w), gradients.dtype),
            vmem((n_col, n_row, ROWS, LANES * COLS), gradients.dtype),
            *[vmem((k, blocks, ROWS, COLS), F32) for k in chunks],
            *[vmem((k, blocks >> s, ROWS, COLS), F32) for k in chunks for s in range(bits + 1)],
            vmem((ROWS, 128), F32),
            vmem((3, 1, 128), jnp.int32),
            vmem((1, 128), F32),
            vmem((devices, 1, 128), F32),
            smem(bucket_lengths.shape, jnp.int32),
            smem(owner_offset.shape, jnp.int32),
            smem(clip_rms.shape, F32),
            dma((2 * n_col,)),
            dma((3,)),
            *[dma((bits + 1,)) for _ in chunks],
            *[dma((sum(plan(bits)[2]),)) for _ in chunks],
            dma((2,)),
        ],
        compiler_params=pltpu.CompilerParams(
            collective_id=0, has_side_effects=True, vmem_limit_bytes=50 * 1024 * 1024
        ),
    )(gradients.reshape(n_row, rows, width), bucket_lengths, owner_offset, clip_rms)
    count = bucket_lengths.shape[0]
    clipped, rms = pl.pallas_call(
        scale,
        out_shape=(jax.ShapeDtypeStruct((rows, w), F32), jax.ShapeDtypeStruct((1, count), F32)),
        in_specs=[pl.BlockSpec(memory_space=vmem)] * 2,
        out_specs=[pl.BlockSpec(memory_space=pltpu.HBM)] * 2,
        scratch_shapes=[vmem((rows, w), F32), vmem((1, count), F32), dma((PARTS + 1,))],
        compiler_params=pltpu.CompilerParams(vmem_limit_bytes=4 * 1024 * 1024),
    )(averaged, stats)
    return clipped, rms[0]


def solution(mesh):
    n_row, n_col = mesh.shape["row"], mesh.shape["col"]
    in_specs = (P(("row", "col"), None, None), P(), P(), P())
    out_specs = (P("row", "col"), P())
    return jax.shard_map(
        functools.partial(shards, n_row, n_col),
        mesh=mesh, in_specs=in_specs, out_specs=out_specs, check_vma=False,
    )
```

```python
import functools

import jax
import jax.numpy as jnp
from jax import lax
from jax.experimental import pallas as pl
from jax.experimental.pallas import tpu as pltpu
from jax.sharding import PartitionSpec as P

MESH = pl.DeviceIdType.MESH
F32 = jnp.float32
ROWS = 16
COLS = 256
LANES = 3
PARTS = 2
INNER = 16
PLACES = (
    (1.08, 1.67, 1.70),
    (3.85, 3.82, 3.33),
    (6.25, 5.64, 6.04),
    (7.90, 7.35, 7.55),
    (10.61, 9.66, 10.24),
)


def split(units):
    even = units * 13 // 40
    return [units - 2 * even, even, even]


def plan(bits):
    places = list(PLACES[:4])
    while len(places) < bits:
        places.append(tuple(p + 1.5 for p in places[-1]))
    places.append(tuple(max(a, b + 1.5) for a, b in zip(PLACES[4], places[-1])))
    events = [(p % 1, s + 1, l, int(p // 1)) for s, row in enumerate(places) for l, p in enumerate(row)]
    spans = [[b - a for a, b in zip(x, y)] for x, y in zip([(0.0,) * LANES] + places, places)]
    rings = [[2 * (int(row[l] // 1) + 1) for row in spans] for l in range(LANES)]
    return sorted(events), rings


def kernel(n_row, n_col, bits, g_ref, off_hbm, out_ref, stat_ref, src, head, *rest):
    sent, rest = rest[:LANES], rest[LANES:]
    sums, rest = [rest[l * (bits + 1) : (l + 1) * (bits + 1)] for l in range(LANES)], rest[LANES * (bits + 1) :]
    acc, mine, slots, off_ref, load_sem, *rest = rest
    sends, recvs, (both,) = rest[:LANES], rest[LANES : 2 * LANES], rest[2 * LANES :]
    events, rings = plan(bits)
    chunks = [s.shape[0] for s in sent]
    blocks = 1 << bits
    devices = n_row * n_col
    _, _, rows, w = src.shape
    width = w * n_col
    across = w // COLS
    row, col = lax.axis_index("row"), lax.axis_index("col")
    core = col % 2
    me = row * n_col + col
    bases = [sum(chunks[:l]) for l in range(LANES)]

    def unit(l, k):
        u = bases[l] + k
        return (u // across) * ROWS, (u % across) * COLS

    small = pltpu.make_async_copy(off_hbm, off_ref, load_sem.at[2])
    small.start()
    for l in range(LANES):
        top, base = unit(l, 0)
        for j in range(n_col):
            part = g_ref.at[:, pl.ds(top, ROWS), pl.ds(j * w + base, COLS)]
            pltpu.make_async_copy(part, head.at[l, j], load_sem.at[0]).start()
    for j in range(n_col):
        pltpu.make_async_copy(g_ref.at[:, :, pl.ds(j * w, w)], src.at[j], load_sem.at[1]).start()

    def turn(value, bit):
        return 1 - 2 * ((value >> bit) % 2)

    def flip(value, bit):
        return value + turn(value, bit) * (1 << bit)

    def peer(dim):
        return (row, flip(col, 1)) if dim == "y" else (flip(row, dim), col)

    high = list(range(2, bits - 1))
    orders = ([1, "xy", "yx"] + high, [0, "y", 1] + high, ["y", 0, 1] + high)

    def target(s, l, k):
        if s == 0:
            return (row, flip(col, 0))
        dim = orders[l][s - 1]
        if dim in ("xy", "yx"):
            pick = k % 2 if dim == "yx" else 1 - k % 2
            return (row + pick * turn(row, 0), col + (1 - pick) * turn(col, 1) * 2)
        return peer(dim)

    barrier = pltpu.get_barrier_semaphore()
    peers = [(row, flip(col, 0))] + [peer(d) for d in [0, "y", 1] + high]
    for other in peers:
        pl.semaphore_signal(barrier, inc=1, device_id=other, device_id_type=MESH)

    def remote(a, b, s, r, dev):
        return pltpu.make_async_remote_copy(
            src_ref=a, dst_ref=b, send_sem=s, recv_sem=r, device_id=dev, device_id_type=MESH
        )

    def copy(s, l, k):
        half = blocks >> s
        a = sent[l].at[k] if s == 0 else sums[l][s - 1].at[k, pl.ds(half, half)]
        at = sum(rings[l][:s]) + k % rings[l][s]
        return remote(a, sums[l][s].at[k], sends[l].at[s], recvs[l].at[at], target(s, l, k))

    def spot(i, l, k):
        flips = {}
        for j, dim in enumerate(orders[l]):
            flips[dim] = (i >> (bits - 1 - j)) % 2
        if "xy" in flips:
            odd = k % 2
            flips[0] = flips["xy"] * (1 - odd) + flips["yx"] * odd
            flips["y"] = flips["yx"] * (1 - odd) + flips["xy"] * odd
        r = 0
        for b in range(bits - 1):
            r = r + (((row >> b) + flips[b]) % 2) * (1 << b)
        return r, (col // 2 + flips["y"]) % 2

    def each(lo, hi, fn):
        if hi - lo <= INNER:
            for i in range(lo, hi):
                fn(i)
        else:

            @pl.loop(0, (hi - lo) // INNER)
            def _(outer):
                for i in range(INNER):
                    fn(lo + outer * INNER + i)

    def piece(l, k, start, r, c, q):
        origin = lax.rem(c + off_ref[r], n_col)
        if start:
            return head[l, origin, r, :, q * 128 : (q + 1) * 128].astype(F32)
        top, base = unit(l, k)
        at = pl.ds(pl.multiple_of(top, ROWS), ROWS)
        return src[origin, r, at, pl.ds(pl.multiple_of(base + q * 128, 128), 128)].astype(F32)

    def convert(l, k, start=False):
        def fill(i):
            r, yd = spot(i, l, k)
            for q in range(COLS // 128):
                sent[l][k, i, :, q * 128 : (q + 1) * 128] = piece(l, k, start, r, yd * 2 + 1 - core, q)

        each(0, blocks, fill)

    def first(l, k, start=False):
        copy(0, l, k).wait_recv()

        def fold(i):
            r, yd = spot(i, l, k)
            for q in range(COLS // 128):
                sums[l][0][k, i, :, q * 128 : (q + 1) * 128] += piece(l, k, start, r, yd * 2 + core, q)

        each(blocks // 2, blocks, fold)
        copy(1, l, k).start()
        each(0, blocks // 2, fold)

    def middle(s, l, k):
        copy(s - 1, l, k).wait_recv()
        half = blocks >> s

        @pl.loop(half, 2 * half, unroll=min(2, half))
        def _(i):
            sums[l][s - 1][k, i] += sums[l][s - 2][k, i]

        copy(s, l, k).start()

        @pl.loop(0, half, unroll=min(2, half))
        def _(i):
            sums[l][s - 1][k, i] += sums[l][s - 2][k, i]

    def finish(l, k):
        copy(bits, l, k).wait_recv()
        top, base = unit(l, k)
        v = (sums[l][bits][k, 0] + sums[l][bits - 1][k, 0]) * (1.0 / devices)
        out_ref[pl.ds(pl.multiple_of(top, ROWS), ROWS), pl.ds(pl.multiple_of(base, COLS), COLS)] = v
        v = v * v
        total = v[:, 0:128]
        for q in range(128, COLS, 128):
            total = total + v[:, q : q + 128]
        here = lax.broadcasted_iota(jnp.int32, acc.shape, 0) + top
        lane = lax.broadcasted_iota(jnp.int32, acc.shape, 1)
        acc[...] += jnp.where(here == lane, jnp.sum(total, axis=1, keepdims=True), 0.0)

    def step(s, l, k):
        if s == 1:
            first(l, k)
        elif s <= bits:
            middle(s, l, k)
        else:
            finish(l, k)

    acc[...] = jnp.zeros_like(acc)
    small.wait()
    pltpu.make_async_copy(head, head, load_sem.at[0]).wait()
    for l in range(LANES):
        convert(l, 0, True)
    pl.semaphore_wait(barrier, len(peers))
    for l in range(LANES):
        copy(0, l, 0).start()
    for l in range(LANES):
        first(l, 0, True)
    pltpu.make_async_copy(src, src, load_sem.at[1]).wait()

    @pl.loop(1, max(chunks[l] + lag for _, _, l, lag in events))
    def _(t):
        for l in range(LANES):

            @pl.when(t < chunks[l])
            def _():
                convert(l, t)
                copy(0, l, t).start()

        for _, s, l, lag in events:

            @pl.when((t >= lag + (1 if s == 1 else 0)) & (t < chunks[l] + lag))
            def _():
                step(s, l, t - lag)

    local = jnp.sum(acc[...], axis=0, keepdims=True)
    mine[...] = local
    slots[me] = local

    def share(mask):
        other = me
        for b in range(bits + 1):
            if (mask >> b) % 2:
                other = flip(other, b)
        return remote(mine, slots.at[me], both.at[0], both.at[1], (other // n_col, other % n_col))

    for mask in range(devices - 1, 0, -1):
        share(mask).start()

    for l in range(LANES):
        for s in range(bits + 1):
            half = blocks >> s
            a = sent[l] if s == 0 else sums[l][s - 1].at[:, pl.ds(half, half)]
            pltpu.make_async_copy(a, a, sends[l].at[s]).wait()

    others = slots.at[pl.ds(0, devices - 1)]
    pltpu.make_async_copy(others, others, both.at[1]).wait()

    for r in range(n_row):
        total = slots[r * n_col]
        for c in range(1, n_col):
            total = total + slots[r * n_col + c]
        stat_ref[pl.ds(r, 1)] = total
    pltpu.make_async_copy(others, others, both.at[0]).wait()


def scale(devices, avg_ref, stat_ref, len_ref, clip_ref, out_hbm, rms_hbm, out, rms, sem):
    rows, w = avg_ref.shape
    n_row, wide = stat_ref.shape
    count = len_ref.shape[1]
    stat = stat_ref[...]
    total = jnp.sum(jnp.sum(stat, axis=0, keepdims=True), axis=1, keepdims=True)
    overall = jnp.sqrt(total / (devices * rows * w))
    clip = clip_ref[0]
    factor = clip / jnp.maximum(overall, clip)
    part = rows // PARTS
    copies = []
    for i in range(PARTS):
        at = pl.ds(i * part, part)
        out[at] = avg_ref[at] * factor
        copies.append(pltpu.make_async_copy(out.at[at], out_hbm.at[at], sem.at[i + 1]))
        copies[-1].start()
    one = lax.broadcasted_iota(jnp.int32, (count, count), 0)
    two = lax.broadcasted_iota(jnp.int32, (count, count), 1)
    lengths = jnp.broadcast_to(len_ref[...].astype(F32), (count, count))
    ends = jnp.sum(jnp.where(two <= one, lengths, 0.0), axis=1, keepdims=True)
    size = jnp.sum(jnp.where(two == one, lengths, 0.0), axis=1, keepdims=True)
    lane = lax.broadcasted_iota(jnp.int32, (count, wide), 1)
    inside = jnp.zeros((count, wide), F32)
    for r in range(n_row):
        ids = (lane + r * rows).astype(F32)
        inside = inside + jnp.where((ids >= ends - size) & (ids < ends), stat[r : r + 1], 0.0)
    squares = jnp.sum(inside, axis=1, keepdims=True)
    column = jnp.sqrt(squares / (jnp.maximum(size, 1.0) * (w * devices // n_row)))
    rms[...] = jnp.sum(jnp.where(two == one, column, 0.0), axis=0, keepdims=True)
    copies.append(pltpu.make_async_copy(rms, rms_hbm, sem.at[0]))
    copies[-1].start()
    for c in copies:
        c.wait()


def shards(n_row, n_col, gradients, bucket_lengths, owner_offset, clip_rms):
    _, total_rows, width = gradients.shape
    rows, w = total_rows // n_row, width // n_col
    devices = n_row * n_col
    bits = devices.bit_length() - 2
    blocks = 1 << bits
    units = rows // ROWS * (w // COLS)
    chunks = split(units)
    wide = -(-rows // 128) * 128
    vmem, smem = pltpu.VMEM, pltpu.SMEM
    dma = pltpu.SemaphoreType.DMA
    averaged, stats = pl.pallas_call(
        functools.partial(kernel, n_row, n_col, bits),
        out_shape=(
            jax.ShapeDtypeStruct((rows, w), F32),
            jax.ShapeDtypeStruct((n_row, wide), F32),
        ),
        in_specs=[pl.BlockSpec(memory_space=pltpu.HBM)] * 2,
        out_specs=[pl.BlockSpec(memory_space=vmem)] * 2,
        scratch_shapes=[
            vmem((n_col, n_row, rows, w), gradients.dtype),
            vmem((LANES, n_col, n_row, ROWS, COLS), gradients.dtype),
            *[vmem((k, blocks, ROWS, COLS), F32) for k in chunks],
            *[vmem((k, blocks >> s, ROWS, COLS), F32) for k in chunks for s in range(bits + 1)],
            vmem((ROWS, wide), F32),
            vmem((1, wide), F32),
            vmem((devices, 1, wide), F32),
            smem(owner_offset.shape, jnp.int32),
            dma((3,)),
            *[dma((bits + 1,)) for _ in chunks],
            *[dma((sum(ring),)) for ring in plan(bits)[1]],
            dma((2,)),
        ],
        compiler_params=pltpu.CompilerParams(
            collective_id=0, has_side_effects=True, vmem_limit_bytes=50 * 1024 * 1024
        ),
    )(gradients.reshape(n_row, rows, width), owner_offset)
    count = bucket_lengths.shape[0]
    clipped, rms = pl.pallas_call(
        functools.partial(scale, devices),
        out_shape=(jax.ShapeDtypeStruct((rows, w), F32), jax.ShapeDtypeStruct((1, count), F32)),
        in_specs=[pl.BlockSpec(memory_space=m) for m in (vmem, vmem, vmem, smem)],
        out_specs=[pl.BlockSpec(memory_space=pltpu.HBM)] * 2,
        scratch_shapes=[vmem((rows, w), F32), vmem((1, count), F32), dma((PARTS + 1,))],
        compiler_params=pltpu.CompilerParams(vmem_limit_bytes=4 * 1024 * 1024),
    )(averaged, stats, bucket_lengths.reshape(1, count), clip_rms)
    return clipped, rms[0]


def solution(mesh):
    n_row, n_col = mesh.shape["row"], mesh.shape["col"]
    in_specs = (P(("row", "col"), None, None), P(), P(), P())
    out_specs = (P("row", "col"), P())
    return jax.shard_map(
        functools.partial(shards, n_row, n_col),
        mesh=mesh, in_specs=in_specs, out_specs=out_specs, check_vma=False,
    )
```

```python
import functools

import jax
import jax.numpy as jnp
from jax import lax
from jax.experimental import pallas as pl
from jax.experimental.pallas import tpu as pltpu
from jax.sharding import PartitionSpec as P

MESH = pl.DeviceIdType.MESH
F32 = jnp.float32
ROWS = 16
COLS = 256
LANES = 3
PARTS = 1
EARLY = 2
INNER = 16
PLACES = (
    (1.08, 1.67, 1.70),
    (3.85, 3.82, 3.33),
    (6.25, 5.64, 6.04),
    (7.90, 7.35, 7.55),
    (10.61, 9.66, 10.24),
)


def split(units):
    even = units * 13 // 40
    return [units - 2 * even, even, even]


def plan(bits):
    places = list(PLACES[:4])
    while len(places) < bits:
        places.append(tuple(p + 1.5 for p in places[-1]))
    places.append(tuple(max(a, b + 1.5) for a, b in zip(PLACES[4], places[-1])))
    events = [(p % 1, s + 1, l, int(p // 1)) for s, row in enumerate(places) for l, p in enumerate(row)]
    spans = [[b - a for a, b in zip(x, y)] for x, y in zip([(0.0,) * LANES] + places, places)]
    rings = [[2 * (int(row[l] // 1) + 1) for row in spans] for l in range(LANES)]
    return sorted(events), rings


def kernel(n_row, n_col, bits, g_ref, off_hbm, out_ref, stat_ref, src, *rest):
    head, rest = rest[:EARLY], rest[EARLY:]
    sent, rest = rest[:LANES], rest[LANES:]
    sums, rest = [rest[l * (bits + 1) : (l + 1) * (bits + 1)] for l in range(LANES)], rest[LANES * (bits + 1) :]
    acc, mine, slots, off_ref, load_sem, begin, *rest = rest
    sends, recvs, (both,) = rest[:LANES], rest[LANES : 2 * LANES], rest[2 * LANES :]
    events, rings = plan(bits)
    chunks = [s.shape[0] for s in sent]
    blocks = 1 << bits
    devices = n_row * n_col
    _, _, rows, w = src.shape
    width = w * n_col
    across = w // COLS
    row, col = lax.axis_index("row"), lax.axis_index("col")
    core = col % 2
    me = row * n_col + col
    bases = [sum(chunks[:l]) for l in range(LANES)]

    def unit(l, k):
        u = bases[l] + k
        return (u // across) * ROWS, (u % across) * COLS

    small = pltpu.make_async_copy(off_hbm, off_ref, load_sem.at[0])
    small.start()
    for k in range(EARLY):
        for l in range(LANES):
            top, base = unit(l, k)
            for j in range(n_col):
                part = g_ref.at[:, pl.ds(top, ROWS), pl.ds(j * w + base, COLS)]
                pltpu.make_async_copy(part, head[k].at[l, j], load_sem.at[2 + k]).start()
    for j in range(n_col):
        pltpu.make_async_copy(g_ref.at[:, :, pl.ds(j * w, w)], src.at[j], load_sem.at[1]).start()

    def turn(value, bit):
        return 1 - 2 * ((value >> bit) % 2)

    def flip(value, bit):
        return value + turn(value, bit) * (1 << bit)

    def peer(dim):
        return (row, flip(col, 1)) if dim == "y" else (flip(row, dim), col)

    high = list(range(2, bits - 1))
    orders = ([1, "xy", "yx"] + high, [0, "y", 1] + high, ["y", 0, 1] + high)

    def target(s, l, k):
        if s == 0:
            return (row, flip(col, 0))
        dim = orders[l][s - 1]
        if dim in ("xy", "yx"):
            pick = k % 2 if dim == "yx" else 1 - k % 2
            return (row + pick * turn(row, 0), col + (1 - pick) * turn(col, 1) * 2)
        return peer(dim)

    barrier = pltpu.get_barrier_semaphore()
    peers = [(row, flip(col, 0))] + [peer(d) for d in [0, "y", 1] + high]
    for other in peers:
        pl.semaphore_signal(barrier, inc=1, device_id=other, device_id_type=MESH)

    def remote(a, b, s, r, dev):
        return pltpu.make_async_remote_copy(
            src_ref=a, dst_ref=b, send_sem=s, recv_sem=r, device_id=dev, device_id_type=MESH
        )

    def copy(s, l, k):
        half = blocks >> s
        a = sent[l].at[k] if s == 0 else sums[l][s - 1].at[k, pl.ds(half, half)]
        at = sum(rings[l][:s]) + k % rings[l][s]
        return remote(a, sums[l][s].at[k], sends[l].at[s], recvs[l].at[at], target(s, l, k))

    def spot(i, l, k):
        flips = {}
        for j, dim in enumerate(orders[l]):
            flips[dim] = (i >> (bits - 1 - j)) % 2
        if "xy" in flips:
            odd = k % 2
            flips[0] = flips["xy"] * (1 - odd) + flips["yx"] * odd
            flips["y"] = flips["yx"] * (1 - odd) + flips["xy"] * odd
        r = 0
        for b in range(bits - 1):
            r = r + (((row >> b) + flips[b]) % 2) * (1 << b)
        return r, (col // 2 + flips["y"]) % 2

    def each(lo, hi, fn):
        if hi - lo <= INNER:
            for i in range(lo, hi):
                fn(i)
        else:

            @pl.loop(0, (hi - lo) // INNER)
            def _(outer):
                for i in range(INNER):
                    fn(lo + outer * INNER + i)

    def piece(l, k, start, r, c, q):
        origin = lax.rem(c + off_ref[r], n_col)
        if start:
            return head[k][l, origin, r, :, q * 128 : (q + 1) * 128].astype(F32)
        top, base = unit(l, k)
        at = pl.ds(pl.multiple_of(top, ROWS), ROWS)
        return src[origin, r, at, pl.ds(pl.multiple_of(base + q * 128, 128), 128)].astype(F32)

    def convert(l, k, start=False, lo=0, hi=blocks):
        def fill(i):
            r, yd = spot(i, l, k)
            for q in range(COLS // 128):
                sent[l][k, i, :, q * 128 : (q + 1) * 128] = piece(l, k, start, r, yd * 2 + 1 - core, q)

        each(lo, hi, fill)

    def halves(l):
        half = blocks // 2
        parts = ((half, begin.at[l]), (0, recvs[l].at[0]))
        return [
            remote(sent[l].at[0, pl.ds(at, half)], sums[l][0].at[0, pl.ds(at, half)], sends[l].at[0], sem, target(0, l, 0))
            for at, sem in parts
        ]

    def first(l, k, start=False):
        if start and k == 0:
            halves(l)[0].wait_recv()
        else:
            copy(0, l, k).wait_recv()

        def fold(i):
            r, yd = spot(i, l, k)
            for q in range(COLS // 128):
                sums[l][0][k, i, :, q * 128 : (q + 1) * 128] += piece(l, k, start, r, yd * 2 + core, q)

        each(blocks // 2, blocks, fold)
        copy(1, l, k).start()
        if start and k == 0:
            halves(l)[1].wait_recv()
        each(0, blocks // 2, fold)

    def middle(s, l, k):
        copy(s - 1, l, k).wait_recv()
        half = blocks >> s

        @pl.loop(half, 2 * half, unroll=min(2, half))
        def _(i):
            sums[l][s - 1][k, i] += sums[l][s - 2][k, i]

        copy(s, l, k).start()

        @pl.loop(0, half, unroll=min(2, half))
        def _(i):
            sums[l][s - 1][k, i] += sums[l][s - 2][k, i]

    def finish(l, k):
        copy(bits, l, k).wait_recv()
        top, base = unit(l, k)
        v = (sums[l][bits][k, 0] + sums[l][bits - 1][k, 0]) * (1.0 / devices)
        out_ref[pl.ds(pl.multiple_of(top, ROWS), ROWS), pl.ds(pl.multiple_of(base, COLS), COLS)] = v
        v = v * v
        total = v[:, 0:128]
        for q in range(128, COLS, 128):
            total = total + v[:, q : q + 128]
        here = lax.broadcasted_iota(jnp.int32, acc.shape, 0) + top
        lane = lax.broadcasted_iota(jnp.int32, acc.shape, 1)
        acc[...] += jnp.where(here == lane, jnp.sum(total, axis=1, keepdims=True), 0.0)

    def step(s, l, k):
        if s == 1:
            first(l, k)
        elif s <= bits:
            middle(s, l, k)
        else:
            finish(l, k)

    acc[...] = jnp.zeros_like(acc)
    small.wait()
    pl.semaphore_wait(barrier, len(peers))
    pltpu.make_async_copy(head[0], head[0], load_sem.at[2]).wait()
    for part, lo in enumerate((blocks // 2, 0)):
        for l in range(LANES):
            convert(l, 0, True, lo, lo + blocks // 2)
            halves(l)[part].start()
    for k in range(1, EARLY):
        pltpu.make_async_copy(head[k], head[k], load_sem.at[2 + k]).wait()
        for l in range(LANES):
            convert(l, k, True)
            copy(0, l, k).start()
    for k in range(EARLY):
        for l in range(LANES):
            first(l, k, True)
    pltpu.make_async_copy(src, src, load_sem.at[1]).wait()

    @pl.loop(EARLY, max(chunks[l] + lag for _, _, l, lag in events))
    def _(t):
        for l in range(LANES):

            @pl.when(t < chunks[l])
            def _():
                convert(l, t)
                copy(0, l, t).start()

        for _, s, l, lag in events:

            @pl.when((t >= lag + (EARLY if s == 1 else 0)) & (t < chunks[l] + lag))
            def _():
                step(s, l, t - lag)

    local = jnp.sum(acc[...], axis=0, keepdims=True)
    mine[...] = local
    slots[me] = local

    def share(mask):
        other = me
        for b in range(bits + 1):
            if (mask >> b) % 2:
                other = flip(other, b)
        return remote(mine, slots.at[me], both.at[0], both.at[1], (other // n_col, other % n_col))

    for mask in range(devices - 1, 0, -1):
        share(mask).start()

    for l in range(LANES):
        for s in range(bits + 1):
            half = blocks >> s
            a = sent[l] if s == 0 else sums[l][s - 1].at[:, pl.ds(half, half)]
            pltpu.make_async_copy(a, a, sends[l].at[s]).wait()

    others = slots.at[pl.ds(0, devices - 1)]
    pltpu.make_async_copy(others, others, both.at[1]).wait()

    for r in range(n_row):
        total = slots[r * n_col]
        for c in range(1, n_col):
            total = total + slots[r * n_col + c]
        stat_ref[pl.ds(r, 1)] = total
    pltpu.make_async_copy(others, others, both.at[0]).wait()


def scale(devices, avg_ref, stat_ref, len_ref, clip_ref, out_hbm, rms_hbm, out, rms, sem):
    rows, w = avg_ref.shape
    n_row, wide = stat_ref.shape
    count = len_ref.shape[1]
    stat = stat_ref[...]
    total = jnp.sum(jnp.sum(stat, axis=0, keepdims=True), axis=1, keepdims=True)
    overall = jnp.sqrt(total / (devices * rows * w))
    clip = clip_ref[0]
    factor = clip / jnp.maximum(overall, clip)
    part = rows // PARTS
    copies = []
    for i in range(PARTS):
        at = pl.ds(i * part, part)
        out[at] = avg_ref[at] * factor
        copies.append(pltpu.make_async_copy(out.at[at], out_hbm.at[at], sem.at[i + 1]))
        copies[-1].start()
    one = lax.broadcasted_iota(jnp.int32, (count, count), 0)
    two = lax.broadcasted_iota(jnp.int32, (count, count), 1)
    lengths = jnp.broadcast_to(len_ref[...].astype(F32), (count, count))
    ends = jnp.sum(jnp.where(two <= one, lengths, 0.0), axis=1, keepdims=True)
    size = jnp.sum(jnp.where(two == one, lengths, 0.0), axis=1, keepdims=True)
    lane = lax.broadcasted_iota(jnp.int32, (count, wide), 1)
    inside = jnp.zeros((count, wide), F32)
    for r in range(n_row):
        ids = (lane + r * rows).astype(F32)
        inside = inside + jnp.where((ids >= ends - size) & (ids < ends), stat[r : r + 1], 0.0)
    squares = jnp.sum(inside, axis=1, keepdims=True)
    column = jnp.sqrt(squares / (jnp.maximum(size, 1.0) * (w * devices // n_row)))
    rms[...] = jnp.sum(jnp.where(two == one, column, 0.0), axis=0, keepdims=True)
    copies.append(pltpu.make_async_copy(rms, rms_hbm, sem.at[0]))
    copies[-1].start()
    for c in copies:
        c.wait()


def shards(n_row, n_col, gradients, bucket_lengths, owner_offset, clip_rms):
    _, total_rows, width = gradients.shape
    rows, w = total_rows // n_row, width // n_col
    devices = n_row * n_col
    bits = devices.bit_length() - 2
    blocks = 1 << bits
    units = rows // ROWS * (w // COLS)
    chunks = split(units)
    wide = -(-rows // 128) * 128
    vmem, smem = pltpu.VMEM, pltpu.SMEM
    dma = pltpu.SemaphoreType.DMA
    averaged, stats = pl.pallas_call(
        functools.partial(kernel, n_row, n_col, bits),
        out_shape=(
            jax.ShapeDtypeStruct((rows, w), F32),
            jax.ShapeDtypeStruct((n_row, wide), F32),
        ),
        in_specs=[pl.BlockSpec(memory_space=pltpu.HBM)] * 2,
        out_specs=[pl.BlockSpec(memory_space=vmem)] * 2,
        scratch_shapes=[
            vmem((n_col, n_row, rows, w), gradients.dtype),
            *[vmem((LANES, n_col, n_row, ROWS, COLS), gradients.dtype)] * EARLY,
            *[vmem((k, blocks, ROWS, COLS), F32) for k in chunks],
            *[vmem((k, blocks >> s, ROWS, COLS), F32) for k in chunks for s in range(bits + 1)],
            vmem((ROWS, wide), F32),
            vmem((1, wide), F32),
            vmem((devices, 1, wide), F32),
            smem(owner_offset.shape, jnp.int32),
            dma((2 + EARLY,)),
            dma((LANES,)),
            *[dma((bits + 1,)) for _ in chunks],
            *[dma((sum(ring),)) for ring in plan(bits)[1]],
            dma((2,)),
        ],
        compiler_params=pltpu.CompilerParams(
            collective_id=0, has_side_effects=True, vmem_limit_bytes=50 * 1024 * 1024
        ),
    )(gradients.reshape(n_row, rows, width), pltpu.with_memory_space_constraint(owner_offset, pltpu.HBM))
    count = bucket_lengths.shape[0]
    clipped, rms = pl.pallas_call(
        functools.partial(scale, devices),
        out_shape=(jax.ShapeDtypeStruct((rows, w), F32), jax.ShapeDtypeStruct((1, count), F32)),
        in_specs=[pl.BlockSpec(memory_space=m) for m in (vmem, vmem, vmem, smem)],
        out_specs=[pl.BlockSpec(memory_space=pltpu.HBM)] * 2,
        scratch_shapes=[vmem((rows, w), F32), vmem((1, count), F32), dma((PARTS + 1,))],
        compiler_params=pltpu.CompilerParams(vmem_limit_bytes=4 * 1024 * 1024),
    )(averaged, stats, bucket_lengths.reshape(1, count), clip_rms)
    return clipped, rms[0]


def solution(mesh):
    n_row, n_col = mesh.shape["row"], mesh.shape["col"]
    in_specs = (P(("row", "col"), None, None), P(), P(), P())
    out_specs = (P("row", "col"), P())
    return jax.shard_map(
        functools.partial(shards, n_row, n_col),
        mesh=mesh, in_specs=in_specs, out_specs=out_specs, check_vma=False,
    )
```

```python
import functools

import jax
import jax.numpy as jnp
from jax import lax
from jax.experimental import pallas as pl
from jax.experimental.pallas import tpu as pltpu
from jax.sharding import PartitionSpec as P

MESH = pl.DeviceIdType.MESH
F32 = jnp.float32
ROWS = 16
COLS = 256
LANES = 3
PARTS = 1
EARLY = 2
INNER = 16
PLACES = (
    (1.08, 1.67, 1.70),
    (3.85, 3.82, 3.33),
    (6.25, 5.64, 6.04),
    (7.90, 7.35, 7.55),
    (10.61, 9.66, 10.24),
)


def split(units):
    even = units * 13 // 40
    return [units - 2 * even, even, even]


def plan(bits):
    places = list(PLACES[:4])
    while len(places) < bits:
        places.append(tuple(p + 1.5 for p in places[-1]))
    places.append(tuple(max(a, b + 1.5) for a, b in zip(PLACES[4], places[-1])))
    events = [(p % 1, s + 1, l, int(p // 1)) for s, row in enumerate(places) for l, p in enumerate(row)]
    spans = [[b - a for a, b in zip(x, y)] for x, y in zip([(0.0,) * LANES] + places, places)]
    rings = [[2 * (int(row[l] // 1) + 1) for row in spans] for l in range(LANES)]
    return sorted(events), rings


def kernel(n_row, n_col, bits, g_ref, off_hbm, out_ref, stat_ref, src, *rest):
    head, rest = rest[:EARLY], rest[EARLY:]
    sent, sums, rest = rest[0], rest[1 : bits + 2], rest[bits + 2 :]
    acc, mine, slots, off_ref, load_sem, begin, *rest = rest
    sends, *recvs, both = rest
    events, rings = plan(bits)
    chunks = split(sent.shape[0])
    blocks = 1 << bits
    devices = n_row * n_col
    _, _, rows, w = src.shape
    width = w * n_col
    across = w // COLS
    row, col = lax.axis_index("row"), lax.axis_index("col")
    core = col % 2
    me = row * n_col + col
    bases = [sum(chunks[:l]) for l in range(LANES)]

    def unit(l, k):
        u = bases[l] + k
        return (u // across) * ROWS, (u % across) * COLS

    small = pltpu.make_async_copy(off_hbm, off_ref, load_sem.at[0])
    small.start()
    for k in range(EARLY):
        for l in range(LANES):
            top, base = unit(l, k)
            for j in range(n_col):
                part = g_ref.at[:, pl.ds(top, ROWS), pl.ds(j * w + base, COLS)]
                pltpu.make_async_copy(part, head[k].at[l, j], load_sem.at[2 + k]).start()
    for j in range(n_col):
        pltpu.make_async_copy(g_ref.at[:, :, pl.ds(j * w, w)], src.at[j], load_sem.at[1]).start()

    def turn(value, bit):
        return 1 - 2 * ((value >> bit) % 2)

    def flip(value, bit):
        return value + turn(value, bit) * (1 << bit)

    def peer(dim):
        return (row, flip(col, 1)) if dim == "y" else (flip(row, dim), col)

    high = list(range(2, bits - 1))
    orders = ([1, "xy", "yx"] + high, [0, "y", 1] + high, ["y", 0, 1] + high)

    def target(s, l, k):
        if s == 0:
            return (row, flip(col, 0))
        dim = orders[l][s - 1]
        if dim in ("xy", "yx"):
            pick = k % 2 if dim == "yx" else 1 - k % 2
            return (row + pick * turn(row, 0), col + (1 - pick) * turn(col, 1) * 2)
        return peer(dim)

    barrier = pltpu.get_barrier_semaphore()
    peers = [(row, flip(col, 0))] + [peer(d) for d in [0, "y", 1] + high]
    for other in peers:
        pl.semaphore_signal(barrier, inc=1, device_id=other, device_id_type=MESH)

    def remote(a, b, s, r, dev):
        return pltpu.make_async_remote_copy(
            src_ref=a, dst_ref=b, send_sem=s, recv_sem=r, device_id=dev, device_id_type=MESH
        )

    def copy(s, l, k):
        half = blocks >> s
        u = bases[l] + k
        a = sent.at[u] if s == 0 else sums[s - 1].at[u, pl.ds(half, half)]
        at = sum(rings[l][:s]) + k % rings[l][s]
        return remote(a, sums[s].at[u], sends.at[s], recvs[l].at[at], target(s, l, k))

    def spot(i, l, k):
        flips = {}
        for j, dim in enumerate(orders[l]):
            flips[dim] = (i >> (bits - 1 - j)) % 2
        if "xy" in flips:
            odd = k % 2
            flips[0] = flips["xy"] * (1 - odd) + flips["yx"] * odd
            flips["y"] = flips["yx"] * (1 - odd) + flips["xy"] * odd
        r = 0
        for b in range(bits - 1):
            r = r + (((row >> b) + flips[b]) % 2) * (1 << b)
        return r, (col // 2 + flips["y"]) % 2

    def each(lo, hi, fn):
        if hi - lo <= INNER:
            for i in range(lo, hi):
                fn(i)
        else:

            @pl.loop(0, (hi - lo) // INNER)
            def _(outer):
                for i in range(INNER):
                    fn(lo + outer * INNER + i)

    def piece(l, k, start, r, c, q):
        origin = lax.rem(c + off_ref[r], n_col)
        if start:
            return head[k][l, origin, r, :, q * 128 : (q + 1) * 128].astype(F32)
        top, base = unit(l, k)
        at = pl.ds(pl.multiple_of(top, ROWS), ROWS)
        return src[origin, r, at, pl.ds(pl.multiple_of(base + q * 128, 128), 128)].astype(F32)

    def convert(l, k, start=False, lo=0, hi=blocks):
        def fill(i):
            r, yd = spot(i, l, k)
            for q in range(COLS // 128):
                sent[bases[l] + k, i, :, q * 128 : (q + 1) * 128] = piece(l, k, start, r, yd * 2 + 1 - core, q)

        each(lo, hi, fill)

    def halves(l):
        half = blocks // 2
        u = bases[l]
        parts = ((half, begin.at[l]), (0, recvs[l].at[0]))
        return [
            remote(sent.at[u, pl.ds(at, half)], sums[0].at[u, pl.ds(at, half)], sends.at[0], sem, target(0, l, 0))
            for at, sem in parts
        ]

    def first(l, k, start=False):
        if start and k == 0:
            halves(l)[0].wait_recv()
        else:
            copy(0, l, k).wait_recv()

        def fold(i):
            r, yd = spot(i, l, k)
            for q in range(COLS // 128):
                sums[0][bases[l] + k, i, :, q * 128 : (q + 1) * 128] += piece(l, k, start, r, yd * 2 + core, q)

        each(blocks // 2, blocks, fold)
        copy(1, l, k).start()
        if start and k == 0:
            halves(l)[1].wait_recv()
        each(0, blocks // 2, fold)

    def middle(s, l, k):
        copy(s - 1, l, k).wait_recv()
        half = blocks >> s

        @pl.loop(half, 2 * half, unroll=min(2, half))
        def _(i):
            sums[s - 1][bases[l] + k, i] += sums[s - 2][bases[l] + k, i]

        copy(s, l, k).start()

        @pl.loop(0, half, unroll=min(2, half))
        def _(i):
            sums[s - 1][bases[l] + k, i] += sums[s - 2][bases[l] + k, i]

    def finish(l, k):
        copy(bits, l, k).wait_recv()
        top, base = unit(l, k)
        v = (sums[bits][bases[l] + k, 0] + sums[bits - 1][bases[l] + k, 0]) * (1.0 / devices)
        out_ref[pl.ds(pl.multiple_of(top, ROWS), ROWS), pl.ds(pl.multiple_of(base, COLS), COLS)] = v
        v = v * v
        total = v[:, 0:128]
        for q in range(128, COLS, 128):
            total = total + v[:, q : q + 128]
        here = lax.broadcasted_iota(jnp.int32, acc.shape, 0) + top
        lane = lax.broadcasted_iota(jnp.int32, acc.shape, 1)
        acc[...] += jnp.where(here == lane, jnp.sum(total, axis=1, keepdims=True), 0.0)

    def step(s, l, k):
        if s == 1:
            first(l, k)
        elif s <= bits:
            middle(s, l, k)
        else:
            finish(l, k)

    acc[...] = jnp.zeros_like(acc)
    small.wait()
    pl.semaphore_wait(barrier, len(peers))
    pltpu.make_async_copy(head[0], head[0], load_sem.at[2]).wait()
    for part, lo in enumerate((blocks // 2, 0)):
        for l in range(LANES):
            convert(l, 0, True, lo, lo + blocks // 2)
            halves(l)[part].start()
    for k in range(1, EARLY):
        pltpu.make_async_copy(head[k], head[k], load_sem.at[2 + k]).wait()
        for l in range(LANES):
            convert(l, k, True)
            copy(0, l, k).start()
    for k in range(EARLY):
        for l in range(LANES):
            first(l, k, True)
    pltpu.make_async_copy(src, src, load_sem.at[1]).wait()

    @pl.loop(EARLY, max(chunks[l] + lag for _, _, l, lag in events))
    def _(t):
        for l in range(LANES):

            @pl.when(t < chunks[l])
            def _():
                convert(l, t)
                copy(0, l, t).start()

        for _, s, l, lag in events:

            @pl.when((t >= lag + (EARLY if s == 1 else 0)) & (t < chunks[l] + lag))
            def _():
                step(s, l, t - lag)

    local = jnp.sum(acc[...], axis=0, keepdims=True)
    mine[...] = local
    slots[me] = local

    def share(mask):
        other = me
        for b in range(bits + 1):
            if (mask >> b) % 2:
                other = flip(other, b)
        return remote(mine, slots.at[me], both.at[0], both.at[1], (other // n_col, other % n_col))

    for mask in range(devices - 1, 0, -1):
        share(mask).start()

    for s in range(bits + 1):
        half = blocks >> s
        a = sent if s == 0 else sums[s - 1].at[:, pl.ds(half, half)]
        pltpu.make_async_copy(a, a, sends.at[s]).wait()

    others = slots.at[pl.ds(0, devices - 1)]
    pltpu.make_async_copy(others, others, both.at[1]).wait()

    for r in range(n_row):
        total = slots[r * n_col]
        for c in range(1, n_col):
            total = total + slots[r * n_col + c]
        stat_ref[pl.ds(r, 1)] = total
    pltpu.make_async_copy(others, others, both.at[0]).wait()


def scale(devices, avg_ref, stat_ref, len_ref, clip_ref, out_hbm, rms_hbm, out, rms, sem):
    rows, w = avg_ref.shape
    n_row, wide = stat_ref.shape
    count = len_ref.shape[1]
    stat = stat_ref[...]
    total = jnp.sum(jnp.sum(stat, axis=0, keepdims=True), axis=1, keepdims=True)
    overall = jnp.sqrt(total / (devices * rows * w))
    clip = clip_ref[0]
    factor = clip / jnp.maximum(overall, clip)
    part = rows // PARTS
    copies = []
    for i in range(PARTS):
        at = pl.ds(i * part, part)
        out[at] = avg_ref[at] * factor
        copies.append(pltpu.make_async_copy(out.at[at], out_hbm.at[at], sem.at[i + 1]))
        copies[-1].start()
    one = lax.broadcasted_iota(jnp.int32, (count, count), 0)
    two = lax.broadcasted_iota(jnp.int32, (count, count), 1)
    lengths = jnp.broadcast_to(len_ref[...].astype(F32), (count, count))
    ends = jnp.sum(jnp.where(two <= one, lengths, 0.0), axis=1, keepdims=True)
    size = jnp.sum(jnp.where(two == one, lengths, 0.0), axis=1, keepdims=True)
    lane = lax.broadcasted_iota(jnp.int32, (count, wide), 1)
    inside = jnp.zeros((count, wide), F32)
    for r in range(n_row):
        ids = (lane + r * rows).astype(F32)
        inside = inside + jnp.where((ids >= ends - size) & (ids < ends), stat[r : r + 1], 0.0)
    squares = jnp.sum(inside, axis=1, keepdims=True)
    column = jnp.sqrt(squares / (jnp.maximum(size, 1.0) * (w * devices // n_row)))
    rms[...] = jnp.sum(jnp.where(two == one, column, 0.0), axis=0, keepdims=True)
    copies.append(pltpu.make_async_copy(rms, rms_hbm, sem.at[0]))
    copies[-1].start()
    for c in copies:
        c.wait()


def shards(n_row, n_col, gradients, bucket_lengths, owner_offset, clip_rms):
    _, total_rows, width = gradients.shape
    rows, w = total_rows // n_row, width // n_col
    devices = n_row * n_col
    bits = devices.bit_length() - 2
    blocks = 1 << bits
    units = rows // ROWS * (w // COLS)
    wide = -(-rows // 128) * 128
    vmem, smem = pltpu.VMEM, pltpu.SMEM
    dma = pltpu.SemaphoreType.DMA
    averaged, stats = pl.pallas_call(
        functools.partial(kernel, n_row, n_col, bits),
        out_shape=(
            jax.ShapeDtypeStruct((rows, w), F32),
            jax.ShapeDtypeStruct((n_row, wide), F32),
        ),
        in_specs=[pl.BlockSpec(memory_space=pltpu.HBM)] * 2,
        out_specs=[pl.BlockSpec(memory_space=vmem)] * 2,
        scratch_shapes=[
            vmem((n_col, n_row, rows, w), gradients.dtype),
            *[vmem((LANES, n_col, n_row, ROWS, COLS), gradients.dtype)] * EARLY,
            vmem((units, blocks, ROWS, COLS), F32),
            *[vmem((units, blocks >> s, ROWS, COLS), F32) for s in range(bits + 1)],
            vmem((ROWS, wide), F32),
            vmem((1, wide), F32),
            vmem((devices, 1, wide), F32),
            smem(owner_offset.shape, jnp.int32),
            dma((2 + EARLY,)),
            dma((LANES,)),
            dma((bits + 1,)),
            *[dma((sum(ring),)) for ring in plan(bits)[1]],
            dma((2,)),
        ],
        compiler_params=pltpu.CompilerParams(
            collective_id=0, has_side_effects=True, vmem_limit_bytes=50 * 1024 * 1024
        ),
    )(gradients.reshape(n_row, rows, width), pltpu.with_memory_space_constraint(owner_offset, pltpu.HBM))
    count = bucket_lengths.shape[0]
    clipped, rms = pl.pallas_call(
        functools.partial(scale, devices),
        out_shape=(jax.ShapeDtypeStruct((rows, w), F32), jax.ShapeDtypeStruct((1, count), F32)),
        in_specs=[pl.BlockSpec(memory_space=m) for m in (vmem, vmem, vmem, smem)],
        out_specs=[pl.BlockSpec(memory_space=pltpu.HBM)] * 2,
        scratch_shapes=[vmem((rows, w), F32), vmem((1, count), F32), dma((PARTS + 1,))],
        compiler_params=pltpu.CompilerParams(vmem_limit_bytes=4 * 1024 * 1024),
    )(averaged, stats, bucket_lengths.reshape(1, count), clip_rms)
    return clipped, rms[0]


def solution(mesh):
    n_row, n_col = mesh.shape["row"], mesh.shape["col"]
    in_specs = (P(("row", "col"), None, None), P(), P(), P())
    out_specs = (P("row", "col"), P())
    return jax.shard_map(
        functools.partial(shards, n_row, n_col),
        mesh=mesh, in_specs=in_specs, out_specs=out_specs, check_vma=False,
    )
```
